32 devices in a mesh: rep: 2 (over z, core), dp: 16 (over x, y).
Axes of the slice: x: 4, y: 4, z: 1, core: 2. Of those that a mesh axis runs over, the one named last changes fastest.
The devices are a block of a 4x4x8 slice.
Arguments:
- x: bfloat16 [32, 1024, 1024], P(('rep', 'dp')), parts along dimension 0
- dy: bfloat16 [32, 1024, 1024], P(('rep', 'dp')), parts along dimension 0
- w_gate: bfloat16 [2, 1024, 3200], replicated
- w_up: bfloat16 [2, 1024, 3200], replicated
- w_down: bfloat16 [2, 3200, 1024], replicated
- m_w_gate: float32 [2, 1024, 3200], replicated
- m_w_up: float32 [2, 1024, 3200], replicated
- m_w_down: float32 [2, 3200, 1024], replicated
- v_w_gate: float32 [2, 1024, 3200], replicated
- v_w_up: float32 [2, 1024, 3200], replicated
- v_w_down: float32 [2, 3200, 1024], replicated
Outputs:
- output 1: bfloat16 [4, 1024, 3200], P('rep'), parts along dimension 0
- output 2: bfloat16 [4, 1024, 3200], P('rep'), parts along dimension 0
- output 3: bfloat16 [4, 3200, 1024], P('rep'), parts along dimension 0
- output 4: float32 [4, 1024, 3200], P('rep'), parts along dimension 0
- output 5: float32 [4, 1024, 3200], P('rep'), parts along dimension 0
- output 6: float32 [4, 3200, 1024], P('rep'), parts along dimension 0
- output 7: float32 [4, 1024, 3200], P('rep'), parts along dimension 0
- output 8: float32 [4, 1024, 3200], P('rep'), parts along dimension 0
- output 9: float32 [4, 3200, 1024], P('rep'), parts along dimension 0
There are 2 independent parts. The reference program is written for one: setup_inputs(seed, part) draws one part's arguments, and reference() takes and returns one part's arrays. A program takes and returns all parts, laid end to end along the dimension named above; an argument that names none is the same for every part.
All inputs are finite; a program needn't handle non-finite values.
Results may differ from the reference program's by a relative error of at most 0.022.
Values are sent between devices in bfloat16 or wider.
A program may use at most 768 MiB of HBM per device.

```python
import jax
import jax.numpy as jnp
from jax import lax

SEQUENCES = 16
TOKENS = 1024
D = 1024
FF = 3200
LAYERS = 2
NAMES = ("w_gate", "w_up", "w_down")
SHAPES = {"w_gate": (LAYERS, D, FF), "w_up": (LAYERS, D, FF), "w_down": (LAYERS, FF, D)}


def bump(key, n, height):
    away = (jnp.arange(n, dtype=jnp.int32) - jax.random.randint(key, (), 0, n, jnp.int32)) % n
    return jnp.where(away < n // 8, height, 1.0)


def together(key, own, strength):
    shared = jax.random.normal(key, own.shape[1:], jnp.float32)
    return (own + strength * shared) * lax.rsqrt(1 + strength * strength)


def setup_inputs(seed: int = 0, part: int = 0) -> dict:
    kx, kdy, ka, kb, kz, kf, kh, kl, *keys = jax.random.split(jax.random.key(seed), 8 + 3 * len(NAMES))
    kx, kdy, ka, kb = (jax.random.fold_in(k, part) for k in (kx, kdy, ka, kb))
    kw, km, kv = (keys[i::3] for i in range(3))
    shape = (SEQUENCES, TOKENS, D)
    much_x, much_dy = jax.random.uniform(kz, (2,), jnp.float32, 0.0, 1.0)
    loud = 2.0 ** jax.random.uniform(jax.random.fold_in(kz, 1), (), jnp.float32, -1.0, 2.0)
    layers = 2.0 ** jax.random.uniform(kl, (LAYERS, 1, 1), jnp.float32, -1.0, 1.0)
    x = together(ka, jax.random.normal(kx, shape, jnp.float32), much_x) * bump(kf, D, 4.0)
    dy = together(kb, jax.random.normal(kdy, shape, jnp.float32), much_dy)
    drawn = {"x": x.astype(jnp.bfloat16), "dy": (loud * dy * (SEQUENCES * TOKENS) ** -0.5).astype(jnp.bfloat16)}
    for key, name in zip(kw, NAMES, strict=True):
        w = jax.random.normal(key, SHAPES[name], jnp.float32) * SHAPES[name][1] ** -0.5
        drawn[name] = (w * {"w_gate": 1.0, "w_up": bump(kh, FF, 4.0), "w_down": layers}[name]).astype(jnp.bfloat16)
    for key, name in zip(km, NAMES, strict=True):
        drawn[f"m_{name}"] = 0.1 * jax.random.normal(key, SHAPES[name], jnp.float32)
    for key, name in zip(kv, NAMES, strict=True):
        drawn[f"v_{name}"] = jax.random.uniform(key, SHAPES[name], jnp.float32, 0.005, 0.015)
    return drawn


def matmul(a, w):
    return jnp.dot(a, w, preferred_element_type=jnp.float32).astype(jnp.bfloat16)


def normed(h):
    wide = h.astype(jnp.float32)
    scale = lax.rsqrt(jnp.mean(wide**2, -1, keepdims=True) + 1e-6)
    return (wide * scale).astype(jnp.bfloat16)


def layer(h, w):
    a = normed(h)
    gate = jnp.dot(a, w["w_gate"], preferred_element_type=jnp.float32)
    up = jnp.dot(a, w["w_up"], preferred_element_type=jnp.float32)
    return h + matmul((jax.nn.silu(gate) * up).astype(jnp.bfloat16), w["w_down"])


def adamw(w, m, v, g):
    m = 0.9 * m + 0.1 * g
    v = 0.95 * v + 0.05 * g * g
    step = m * lax.rsqrt(v + 1e-8) + 0.1 * w
    return (w - 0.02 * step).astype(jnp.bfloat16), m, v


def stack(weights, h):
    return lax.scan(lambda h, w: (layer(h, w), None), h, weights)[0]


def reference(x, dy, w_gate, w_up, w_down, m_w_gate, m_w_up, m_w_down, v_w_gate, v_w_up, v_w_down):
    weights = dict(zip(NAMES, (w_gate, w_up, w_down), strict=True))

    def take(so_far, sequence):
        h, by_y = sequence
        _, back = jax.vjp(lambda w: stack(w, h), weights)
        return jax.tree.map(lambda total, term: total + term.astype(jnp.float32), so_far, back(by_y)[0]), None

    none_yet = {name: jnp.zeros(w.shape, jnp.float32) for name, w in weights.items()}
    by_weights, _ = lax.scan(take, none_yet, (x, dy))
    gradients = [by_weights[name].astype(jnp.bfloat16).astype(jnp.float32) for name in NAMES]
    new = [
        adamw(w.astype(jnp.float32), m, v, g)
        for w, m, v, g in zip((w_gate, w_up, w_down), (m_w_gate, m_w_up, m_w_down), (v_w_gate, v_w_up, v_w_down), gradients, strict=True)
    ]
    return tuple(one[which] for which in range(3) for one in new)
```

```python
import functools
import math

import jax
import jax.numpy as jnp
from jax import lax
from jax.experimental import pallas as pl
from jax.experimental.pallas import tpu as pltpu
from jax.sharding import PartitionSpec as P

BF, F32 = jnp.bfloat16, jnp.float32
MESH = pl.DeviceIdType.MESH
COLOURS = 4
LANES = 128
BLOCK = 640
TILE = 256
TERMS, EARLY, LAST = 4, 3, 5
NN, NT, TN = ((((1,), (0,)), ((), ())), (((1,), (1,)), ((), ())), (((0,), (0,)), ((), ())))


def dot(a, b, dims=NN):
    return lax.dot_general(a, b, dims, preferred_element_type=F32)


def rms(wide):
    return lax.rsqrt(jnp.mean(wide * wide, -1, keepdims=True) + 1e-6)


def forward_kernel(h_ref, wg_ref, wu_ref, wd_ref, out_ref, a_ref, acc_ref, wgu, wd, sems, *, number):
    d, ff = wg_ref.shape[1:]
    blocks = ff // BLOCK
    tokens = h_ref.shape[0]

    def load(f, slot):
        cols = pl.ds(pl.multiple_of(f * BLOCK, BLOCK), BLOCK)
        return (
            pltpu.make_async_copy(wg_ref.at[number, :, cols], wgu.at[slot, :, pl.ds(0, BLOCK)], sems.at[0, slot]),
            pltpu.make_async_copy(wu_ref.at[number, :, cols], wgu.at[slot, :, pl.ds(BLOCK, BLOCK)], sems.at[1, slot]),
            pltpu.make_async_copy(wd_ref.at[number, cols], wd.at[slot], sems.at[2, slot]),
        )

    for copy in load(0, 0):
        copy.start()
    wide = h_ref[...].astype(F32)
    a_ref[...] = (wide * rms(wide)).astype(BF)
    acc_ref[...] = jnp.zeros_like(acc_ref)

    def block(f, _):
        slot = lax.rem(f, 2)
        for copy in load(f, slot):
            copy.wait()

        @pl.when(f + 1 < blocks)
        def _():
            for copy in load(f + 1, 1 - slot):
                copy.start()

        for r in range(tokens // TILE):
            rows = pl.ds(r * TILE, TILE)
            both = dot(a_ref[rows, :], wgu[slot])
            gate, up = both[:, :BLOCK], both[:, BLOCK:]
            mid = (gate * jax.nn.sigmoid(gate) * up).astype(BF)
            acc_ref[rows, :] += dot(mid, wd[slot])
        return 0

    lax.fori_loop(0, blocks, block, 0)
    out_ref[...] = (h_ref[...].astype(F32) + acc_ref[...].astype(BF).astype(F32)).astype(BF)


def forward(h, wg, wu, wd, number):
    t, d = h.shape
    ff = wg.shape[2]
    any_spec = pl.BlockSpec(memory_space=pl.ANY)
    vmem = pl.BlockSpec(memory_space=pltpu.VMEM)
    return pl.pallas_call(
        functools.partial(forward_kernel, number=number),
        in_specs=[vmem, any_spec, any_spec, any_spec],
        out_specs=vmem,
        out_shape=jax.ShapeDtypeStruct((t, d), BF),
        scratch_shapes=[
            pltpu.VMEM((t, d), BF),
            pltpu.VMEM((t, d), F32),
            pltpu.VMEM((2, d, 2 * BLOCK), BF),
            pltpu.VMEM((2, BLOCK, d), BF),
            pltpu.SemaphoreType.DMA((3, 2)),
        ],
        compiler_params=pltpu.CompilerParams(vmem_limit_bytes=56 << 20),
        name="forward",
        cost_estimate=pl.CostEstimate(flops=6 * t * d * ff, bytes_accessed=6 * d * ff, transcendentals=0),
    )(h, wg, wu, wd)


def backward_kernel(*refs, layers, side):
    hs, (dy_ref, wg_ref, wu_ref, wd_ref), refs = refs[:layers], refs[layers : layers + 4], refs[layers + 4 :]
    own = [refs[i * COLOURS : (i + 1) * COLOURS] for i in range(layers)]
    refs = refs[layers * COLOURS :]
    h_v, a_v, at_v, by_v, acc_v, wgu, wd, mid_v, dgu_v, terms, early, last, second = refs[:13]
    w_sem, l_sem, a_send, a_recv, b_send, b_recv, o_sem, g_send, g_recv, a_free, b_free = refs[13:]
    tokens, d = h_v.shape
    blocks = wg_ref.shape[2] // BLOCK
    chunks = layers * blocks
    step_rows = d // (COLOURS * side * side)
    me = lax.axis_index("dp")
    pos = (me // side, lax.rem(me, side))

    def at(axis, by):
        moved = lax.rem(pos[axis] + by + 2 * side, side)
        return {"dp": moved * side + pos[1] if axis == 0 else pos[0] * side + moved}

    def way(c):
        return c // 2, 1 - 2 * (c % 2)

    def place(axis, by):
        return lax.rem(pos[axis] + by + 4 * side, side)

    barrier = pltpu.get_barrier_semaphore()
    for axis in range(2):
        for by in (1, -1):
            pl.semaphore_signal(barrier, inc=1, device_id=at(axis, by), device_id_type=MESH)
    pl.semaphore_wait(barrier, 4)

    def a_copy(step, k, c):
        axis, sign = way(c)
        src = terms.at[lax.rem(k, TERMS), c, place(axis, -sign)] if step == 0 else early.at[step - 1, lax.rem(k, EARLY), c]
        dst = last.at[lax.rem(k, LAST), c] if step == 2 else early.at[step, lax.rem(k, EARLY), c]
        slot = lax.rem(k, LAST if step == 2 else EARLY)
        return pltpu.make_async_remote_copy(
            src_ref=src,
            dst_ref=dst,
            send_sem=a_send.at[step, lax.rem(k, EARLY), c],
            recv_sem=a_recv.at[step, slot, c],
            device_id=at(axis, sign),
            device_id_type=MESH,
        )

    def b_copy(step, k, c):
        axis, sign = way(c)
        slot = lax.rem(k, EARLY)
        src = last.at[lax.rem(k, LAST), c, place(1 - axis, -sign)] if step == 0 else second.at[step - 1, slot, c]
        return pltpu.make_async_remote_copy(
            src_ref=src,
            dst_ref=second.at[step, slot, c],
            send_sem=b_send.at[step, slot, c],
            recv_sem=b_recv.at[step, slot, c],
            device_id=at(1 - axis, sign),
            device_id_type=MESH,
        )

    def own_copy(k, c, half):
        axis, _ = way(c)
        slot = lax.rem(k, EARLY)
        return pltpu.make_async_copy(second.at[2, slot, c], own[half][c].at[lax.rem(k, blocks), pos[1 - axis]], o_sem.at[slot, c])

    def start(copy, free, k, slots):
        @pl.when(k >= slots)
        def _():
            pl.semaphore_wait(free, 1)

        copy.start()

    def give(free, k, slots, axis, by):
        @pl.when(k + slots < chunks)
        def _():
            pl.semaphore_signal(free, inc=1, device_id=at(axis, by), device_id_type=MESH)

    def add(total, term):
        parts = total.shape[0]

        def one(i, _):
            total[i] = (total[i].astype(F32) + term[i].astype(F32)).astype(BF)
            return 0

        lax.fori_loop(0, parts, one, 0, unroll=True if parts == 3 else 2)

    def service(step, k):
        @pl.when((k >= 0) & (k < chunks))
        def _():
            if step == 0:
                for c in range(COLOURS):
                    start(a_copy(0, k, c), a_free.at[0, c], k, EARLY)
            elif step < 4:
                for c in range(COLOURS):
                    axis, sign = way(c)
                    a_copy(step - 1, k, c).wait_recv()
                    if step >= 2:
                        if step == 2:
                            a_copy(0, k, c).wait_send()
                        a_copy(step - 1, k, c).wait_send()
                        give(a_free.at[step - 2, c], k, EARLY, axis, -sign)
                    total = last.at[lax.rem(k, LAST), c] if step == 3 else early.at[step - 1, lax.rem(k, EARLY), c]
                    term = terms.at[lax.rem(k, TERMS), c, place(axis, -(step + 1) * sign)]
                    for s in range(side):
                        add(total.at[s], term.at[s])
                    if c:
                        a_next(step, k, c - 1)
                a_next(step, k, COLOURS - 1)
            elif step < 7:
                stage = step - 4
                for c in range(COLOURS):
                    axis, sign = way(c)
                    b_copy(stage, k, c).wait_recv()
                    if stage >= 1:
                        if stage == 1:
                            b_copy(0, k, c).wait_send()
                        b_copy(stage, k, c).wait_send()
                        give(b_free.at[stage - 1, c], k, EARLY, 1 - axis, -sign)
                    add(second.at[stage, lax.rem(k, EARLY), c], last.at[lax.rem(k, LAST), c, place(1 - axis, -(stage + 2) * sign)])
                    if c:
                        b_next(stage, k, c - 1)
                b_next(stage, k, COLOURS - 1)
            else:
                for c in range(COLOURS):
                    axis, sign = way(c)
                    own_copy(k, c, 0).wait()
                    give(b_free.at[2, c], k, EARLY, 1 - axis, -sign)

    def a_next(step, k, c):
        if step < 3:
            start(a_copy(step, k, c), a_free.at[step, c], k, LAST if step == 2 else EARLY)
        else:
            start(b_copy(0, k, c), b_free.at[0, c], k, EARLY)

    def b_next(stage, k, c):
        axis, sign = way(c)
        if stage < 2:
            start(b_copy(stage + 1, k, c), b_free.at[stage + 1, c], k, EARLY)
        else:
            give(a_free.at[2, c], k, LAST, axis, -sign)
            for half in range(layers):

                @pl.when(k // blocks == half)
                def _(half=half):
                    own_copy(k, c, half).start()


    def g_copy(step, half, c):
        axis, sign = way(c)
        part = own[half][c].at[:, place(1 - axis, -step * sign)]
        return pltpu.make_async_remote_copy(
            src_ref=part,
            dst_ref=part,
            send_sem=g_send.at[step, half, c],
            recv_sem=g_recv.at[step, half, c],
            device_id=at(1 - axis, sign),
            device_id_type=MESH,
        )

    def bring(step, half):
        for c in range(COLOURS):
            if step > 0:
                g_copy(step - 1, half, c).wait_recv()
            if step < side - 1:
                g_copy(step, half, c).start()

    def load(w, slot):
        number = layers - 1 - w // blocks
        cols = pl.ds(pl.multiple_of(lax.rem(w, blocks) * BLOCK, BLOCK), BLOCK)
        return (
            pltpu.make_async_copy(wg_ref.at[number, :, cols], wgu.at[slot, :, pl.ds(0, BLOCK)], w_sem.at[0, slot]),
            pltpu.make_async_copy(wu_ref.at[number, :, cols], wgu.at[slot, :, pl.ds(BLOCK, BLOCK)], w_sem.at[1, slot]),
            pltpu.make_async_copy(wd_ref.at[number, cols], wd.at[slot], w_sem.at[2, slot]),
        )

    def load_h(half):
        return pltpu.make_async_copy(hs[layers - 1 - half], h_v, l_sem.at[0])

    pieces = tokens // TILE
    for copy in load(0, 0):
        copy.start()
    load_h(0).start()
    first = pltpu.make_async_copy(dy_ref, by_v, l_sem.at[1])
    first.start()
    first.wait()

    for half in range(layers):
        load_h(half).wait()
        for r in range(pieces):
            rows = pl.ds(r * TILE, TILE)
            wide = h_v[rows, :].astype(F32)
            a = wide * rms(wide)
            a_v[rows, :] = a.astype(BF)
            at_v[:, rows] = a.T.astype(BF)
        if half + 1 < layers:
            acc_v[...] = jnp.zeros_like(acc_v)

        def round_(f, _, half=half):
            k = half * blocks + f
            slot = lax.rem(k, 2)
            mine = lax.rem(k, TERMS)
            for copy in load(k, slot):
                copy.wait()

            @pl.when(k + 1 < chunks)
            def _():
                for copy in load(k + 1, 1 - slot):
                    copy.start()

            for r in range(pieces):
                rows = pl.ds(r * TILE, TILE)
                both = dot(a_v[rows, :], wgu[slot])
                gate, up = both[:, :BLOCK], both[:, BLOCK:]
                back = dot(by_v[rows, :], wd[slot], NT).astype(BF).astype(F32)
                gone = jax.nn.sigmoid(gate)
                silu = gate * gone
                mid_v[rows, :] = (silu * up).astype(BF)
                dgu_v[rows, pl.ds(0, BLOCK)] = (back * up * (gone * (1 + gate * (1 - gone)))).astype(BF)
                dgu_v[rows, pl.ds(BLOCK, BLOCK)] = (back * silu).astype(BF)
                service(1 + r, k - 1 - r)
            down = dot(mid_v[...], by_v[...], TN)
            each = BLOCK // (side * side * 8)
            for c in range(COLOURS):
                two = [down[:, (2 * c + t) * LANES : (2 * c + t + 1) * LANES].reshape(side, side, each, 8, LANES) for t in range(2)]
                terms[mine, c, :, :, 2] = jnp.stack(two, 3).reshape(side, side, 2 * each * 8, LANES).astype(BF)
            service(5, k - 5)
            for c in range(COLOURS):
                part = dot(at_v[c * d // COLOURS : (c + 1) * d // COLOURS, :], dgu_v[...])
                for m in range(2):
                    for j in range(BLOCK // LANES):
                        col = m * BLOCK + j * LANES
                        terms[mine, c, :, :, m, j * step_rows : (j + 1) * step_rows, :] = (
                            part[:, col : col + LANES].reshape(side, side, step_rows, LANES).astype(BF)
                        )
                if c % 2:
                    service(6 + c // 2, k - 6 - c // 2)
            service(0, k)
            if half + 1 < layers:
                for r in range(pieces):
                    rows = pl.ds(r * TILE, TILE)
                    acc_v[rows, :] += dot(dgu_v[rows, :], wgu[slot], NT)
            return 0

        lax.fori_loop(0, blocks, round_, 0)
        if half + 1 < layers:
            for r in range(pieces):
                rows = pl.ds(r * TILE, TILE)
                wide = h_v[rows, :].astype(F32)
                scale = rms(wide)
                g = acc_v[rows, :].astype(BF).astype(F32)
                along = jnp.sum(g * wide, -1, keepdims=True) * (scale * scale * scale / d)
                back = (scale * g - wide * along).astype(BF).astype(F32)
                by_v[rows, :] = (by_v[rows, :].astype(F32) + back).astype(BF)
            load_h(half + 1).start()

    def drain(k, _):
        for step in range(1, 8):
            service(step, k - step)
        for half in range(layers - 1):
            for step in range(side):

                @pl.when(k == (half + 1) * blocks - 1 + 8 + step)
                def _():
                    bring(step, half)

        return 0

    rounds = chunks + 7
    lax.fori_loop(chunks, rounds, drain, 0)
    for half in range(layers):
        for step in range(side):
            if half == layers - 1 or (half + 1) * blocks - 1 + 8 + step >= rounds:
                bring(step, half)
    for half in range(layers):
        for c in range(COLOURS):
            for step in range(side - 1):
                g_copy(step, half, c).wait_send()


def backward(hs, dy, wg, wu, wd, side):
    layers, d, ff = wg.shape
    tokens = dy.shape[0]
    blocks = ff // BLOCK
    rows = BLOCK // LANES * (d // (COLOURS * side * side))
    block = (blocks, side, 3, rows, LANES)
    any_spec = pl.BlockSpec(memory_space=pl.ANY)
    dma = pltpu.SemaphoreType.DMA
    out = pl.pallas_call(
        functools.partial(backward_kernel, layers=layers, side=side),
        in_specs=[any_spec] * (layers + 4),
        out_specs=[any_spec] * (COLOURS * layers),
        out_shape=[jax.ShapeDtypeStruct(block, BF)] * (COLOURS * layers),
        scratch_shapes=[
            pltpu.VMEM((tokens, d), BF),
            pltpu.VMEM((tokens, d), BF),
            pltpu.VMEM((d, tokens), BF),
            pltpu.VMEM((tokens, d), BF),
            pltpu.VMEM((tokens, d), F32),
            pltpu.VMEM((2, d, 2 * BLOCK), BF),
            pltpu.VMEM((2, BLOCK, d), BF),
            pltpu.VMEM((tokens, BLOCK), BF),
            pltpu.VMEM((tokens, 2 * BLOCK), BF),
            pltpu.VMEM((TERMS, COLOURS, side, side, 3, rows, LANES), BF),
            pltpu.VMEM((2, EARLY, COLOURS, side, 3, rows, LANES), BF),
            pltpu.VMEM((LAST, COLOURS, side, 3, rows, LANES), BF),
            pltpu.VMEM((3, EARLY, COLOURS, 3, rows, LANES), BF),
            dma((3, 2)),
            dma((2,)),
            dma((3, EARLY, COLOURS)),
            dma((3, LAST, COLOURS)),
            dma((3, EARLY, COLOURS)),
            dma((3, EARLY, COLOURS)),
            dma((EARLY, COLOURS)),
            dma((side - 1, layers, COLOURS)),
            dma((side - 1, layers, COLOURS)),
            pltpu.SemaphoreType.REGULAR((3, COLOURS)),
            pltpu.SemaphoreType.REGULAR((3, COLOURS)),
        ],
        compiler_params=pltpu.CompilerParams(vmem_limit_bytes=67_043_328, collective_id=0, has_side_effects=True),
        name="backward",
        cost_estimate=pl.CostEstimate(flops=16 * layers * tokens * d * ff, bytes_accessed=12 * layers * d * ff, transcendentals=0),
    )(*hs, dy, wg, wu, wd)
    return [out[i * COLOURS : (i + 1) * COLOURS] for i in range(layers)]


DEPTH = 3


def adamw_kernel(places, *refs, number, side):
    g_refs, src, refs = refs[:COLOURS], refs[COLOURS : COLOURS + 9], refs[-18:]
    dst, (g_v, wide_w, wide_f, wide_nw, wide_nf, tall_w, tall_f, in_sem, out_sem) = refs[:9], refs[9:]
    d, ff = src[0].shape[1:]
    blocks = ff // BLOCK
    wide, tall = d // (COLOURS * side), BLOCK // side
    units = [(c, i) for c in range(COLOURS) for i in range(3)]

    def part(ref, c, i):
        if i < 2:
            return ref.at[number, pl.ds(pl.multiple_of((c * side + places[c]) * wide, wide), wide)]
        return ref.at[number, :, pl.ds(pl.multiple_of(places[c] * tall, tall), tall), pl.ds(c * d // COLOURS, d // COLOURS)]

    def buffers(u, way):
        c, i = units[u]
        if i < 2:
            slot = (2 * c + i) % DEPTH
            w, f = ((wide_w, wide_f), (wide_nw, wide_nf))[way]
            return w.at[slot], f.at[slot, 0], f.at[slot, 1]
        return tall_w.at[way, c % 2], tall_f.at[way, c % 2, 0], tall_f.at[way, c % 2, 1]

    def loads(u):
        c, i = units[u]
        copies = [
            pltpu.make_async_copy(part(src[3 * kind + i], c, i), buffer, in_sem.at[u, kind]) for kind, buffer in enumerate(buffers(u, 0))
        ]
        return copies + [pltpu.make_async_copy(g_refs[c].at[:, :, i], g_v.at[u % DEPTH], in_sem.at[u, 3])]

    def stores(u):
        c, i = units[u]
        return [
            pltpu.make_async_copy(buffer, part(dst[3 * kind + i], c, i), out_sem.at[u, kind]) for kind, buffer in enumerate(buffers(u, 1))
        ]

    for u in range(DEPTH - 1):
        for copy in loads(u):
            copy.start()
    waited = set()
    for u, (c, i) in enumerate(units):
        if u + DEPTH - 1 < len(units):
            for copy in loads(u + DEPTH - 1):
                copy.start()
        for copy in loads(u):
            copy.wait()
        for before in range(u):
            if before not in waited and (i < 2) == (units[before][1] < 2):
                n = lambda unit: 2 * unit[0] + unit[1] if unit[1] < 2 else unit[0]
                if n(units[u]) - n(units[before]) >= (DEPTH if i < 2 else 2):
                    waited.add(before)
                    for copy in stores(before):
                        copy.wait()
        (w_in, m_in, v_in), (w_out, m_out, v_out) = buffers(u, 0), buffers(u, 1)

        def one(where, g):
            m = 0.9 * m_in[where] + 0.1 * g
            v = 0.95 * v_in[where] + 0.05 * g * g
            w = w_in[where].astype(F32)
            step = m * lax.rsqrt(v + 1e-8) + 0.1 * w
            w_out[where] = (w - 0.02 * step).astype(BF)
            m_out[where] = m
            v_out[where] = v

        def block(f, _):
            if i < 2:
                height = wide // side
                for j in range(BLOCK // LANES):
                    g = g_v[u % DEPTH, f, :, j * height : (j + 1) * height, :].astype(F32).reshape(wide, LANES)
                    one((slice(None), pl.ds(pl.multiple_of(f * BLOCK + j * LANES, LANES), LANES)), g)
            else:
                g = g_v[u % DEPTH, f].astype(F32).reshape(tall // 8, 2, 8, LANES)
                for t in range(2):
                    one((f, slice(None), slice(t * LANES, (t + 1) * LANES)), g[:, t].reshape(tall, LANES))
            return 0

        lax.fori_loop(0, blocks, block, 0)
        for copy in stores(u):
            copy.start()
    for u in range(len(units)):
        if u not in waited:
            for copy in stores(u):
                copy.wait()


def adamw(places, gs, weights, ms, vs, number, before, side):
    layers, d, ff = weights[0].shape
    blocks = ff // BLOCK
    rows = gs[0].shape[-2]
    wide, tall = d // (COLOURS * side), BLOCK // side
    arrays = [a.reshape(layers, blocks, BLOCK, d) if i == 2 else a for group in (weights, ms, vs) for i, a in enumerate(group)]
    more = () if before is None else tuple(before)
    any_spec = pl.BlockSpec(memory_space=pl.ANY)
    return pl.pallas_call(
        functools.partial(adamw_kernel, number=number, side=side),
        in_specs=[pl.BlockSpec(memory_space=pltpu.SMEM)] + [any_spec] * (COLOURS + 9 + len(more)),
        out_specs=[any_spec] * 9,
        out_shape=[jax.ShapeDtypeStruct(a.shape, a.dtype) for a in arrays],
        input_output_aliases={1 + COLOURS + 9 + i: i for i in range(len(more))},
        scratch_shapes=[
            pltpu.VMEM((DEPTH, blocks, side, rows, LANES), BF),
            pltpu.VMEM((DEPTH, wide, ff), BF),
            pltpu.VMEM((DEPTH, 2, wide, ff), F32),
            pltpu.VMEM((DEPTH, wide, ff), BF),
            pltpu.VMEM((DEPTH, 2, wide, ff), F32),
            pltpu.VMEM((2, 2, blocks, tall, d // COLOURS), BF),
            pltpu.VMEM((2, 2, 2, blocks, tall, d // COLOURS), F32),
            pltpu.SemaphoreType.DMA((3 * COLOURS, 4)),
            pltpu.SemaphoreType.DMA((3 * COLOURS, 3)),
        ],
        compiler_params=pltpu.CompilerParams(vmem_limit_bytes=63 << 20),
        name="adamw",
        cost_estimate=pl.CostEstimate(flops=d * ff * 1000, bytes_accessed=d * ff * 66 // side, transcendentals=0),
    )(places, *gs, *arrays, *more)


def solution(mesh):
    size = mesh.shape["dp"]
    side = math.isqrt(size)

    def step(x, dy, *arrays):
        weights, ms, vs = (arrays[i : i + 3] for i in (0, 3, 6))
        layers = weights[0].shape[0]
        hs = [x[0]]
        for number in range(layers - 1):
            hs.append(forward(hs[-1], *weights, number))
        own = backward(hs, dy[0], *weights, side)

        me = lax.axis_index("dp")
        pos = (me // side, me % side)

        def along(axis, by):
            pairs = []
            for i in range(size):
                x_, y_ = i // side, i % side
                pairs.append((i, (x_ + by) % side * side + y_ if axis == 0 else x_ * side + (y_ + by) % side))
            return pairs

        def places(distance):
            return jnp.stack([(pos[c // 2] - distance * (1 - 2 * (c % 2)) + side) % side for c in range(COLOURS)]).astype(jnp.int32)

        new, parts = None, [own]
        for distance in range(1, side):
            parts.append([[lax.ppermute(g, "dp", along(c // 2, 1 - 2 * (c % 2))) for c, g in enumerate(half)] for half in parts[-1]])
        for distance in range(side):
            for half in range(layers):
                new = adamw(places(distance), parts[distance][half], weights, ms, vs, layers - 1 - half, new, side)
        return tuple(one.reshape(a.shape) for one, a in zip(new, arrays, strict=True))

    return jax.shard_map(
        step,
        mesh=mesh,
        in_specs=(P(("rep", "dp"), None, None),) * 2 + (P(None, None, None),) * 9,
        out_specs=(P("rep", None, None),) * 9,
        check_vma=False,
    )
```
